32 devices in a mesh: gx: 4 (over z), gy: 4 (over x, core), gz: 2 (over y).
Axes of the slice: x: 2, y: 2, z: 4, core: 2. Of those that a mesh axis runs over, the one named last changes fastest.
Arguments:
- inputs: bfloat16 [112, 112, 14, 96], P('gx', 'gy', 'gz'), may hold values from -6 to 6
- d_out: bfloat16 [112, 112, 14, 96], P('gx', 'gy', 'gz'), may hold values from -6 to 6
- layer_norm_gain: float32 [96], replicated, may hold values from 0.1 to 1.9
- layer_norm_bias: float32 [96], replicated, may hold values from -3 to 3
- w_qkv: bfloat16 [96, 288], replicated, may hold values from -0.625 to 0.625
- b_qkv: float32 [288], replicated, may hold values from -3 to 3
- w_proj: bfloat16 [96, 96], replicated, may hold values from -0.625 to 0.625
- rel_bias: float32 [3, 2197], replicated, may hold values from -4 to 240
Outputs:
- d_x: bfloat16 [112, 112, 14, 96], P('gx', 'gy', 'gz')
- g_qkv: float32 [96, 288], replicated
- g_bqkv: float32 [288], replicated
- g_proj: float32 [96, 96], replicated
- g_rel: float32 [3, 2197], replicated
- gain_gradient: float32 [96], replicated
- g_shift: float32 [96], replicated
The draws below stay inside these ranges and needn't reach their ends.
All inputs are finite; a program needn't handle non-finite values.
Results may differ from the reference program's by a relative error of at most 0.011.
Values may be sent and summed in bfloat16 or wider, within the bound.
No kernel may reach another device: no remote copies, remote signals or barrier semaphores. Data moves between devices by JAX's collectives and lax.ppermute only.
A program may use at most 192 MiB of HBM per device.

```python
import jax
import jax.numpy as jnp
import numpy as np
from jax import lax

C = 96
HEADS = 3
WIN = 7
SHIFT = 3
NX = 112
NY = 112
NZ = 14
TOKENS = 175616
TABLE = 2197


def draw_rel_bias(key, part):
    first = jax.random.fold_in(jax.random.fold_in(key, 17), 0)
    width = 2 * WIN - 1
    return jnp.clip(jax.random.normal(first, (HEADS, width ** 3), jnp.float32), -4.0, 4.0)


def shard_levels(rng, extent, shards, low, high):
    def one(axis_at, shards_of):
        steps = jax.random.uniform(jax.random.fold_in(jax.random.fold_in(rng, 6), axis_at), (shards_of,), jnp.float32, low / len(shards), high / len(shards))
        return jnp.repeat(jnp.exp(steps), extent[axis_at] // shards_of).reshape((-1,) + (1,) * (len(extent) - axis_at - 1))

    loudness = one(*shards[0])
    for cut in shards[1:]:
        loudness = loudness * one(*cut)
    return loudness


def scatter_about(stream_key, extent, spread, reach, pieces=(), dtype=jnp.bfloat16):
    result = spread * jax.random.normal(stream_key, extent, jnp.float32)
    if pieces:
        result = result * shard_levels(stream_key, extent, pieces, -0.22, 0.18)
    return jnp.clip(result, -reach, reach).astype(dtype)


def setup_inputs(seed: int = 0) -> dict:
    key_list = jax.random.split(jax.random.key(seed), 9)
    return {
        "inputs": scatter_about(key_list[0], (NX, NY, NZ, C), 1.0, 6.0, ((0, 4), (1, 4), (2, 2))),
        "d_out": scatter_about(key_list[1], (NX, NY, NZ, C), 1.0, 6.0, ((0, 4), (1, 4), (2, 2))),
        "layer_norm_gain": jnp.clip(1.0 + 0.18 * jax.random.normal(key_list[2], (C,), jnp.float32), 0.1, 1.9),
        "layer_norm_bias": scatter_about(key_list[3], (C,), 0.5, 3.0, (), jnp.float32),
        "w_qkv": scatter_about(key_list[4], (C, 3 * C), C ** -0.5, 0.625),
        "b_qkv": scatter_about(key_list[5], (3 * C,), 0.5, 3.0, (), jnp.float32),
        "w_proj": scatter_about(key_list[6], (C, C), C ** -0.5, 0.625),
        "rel_bias": draw_rel_bias(jax.random.fold_in(key_list[8], 71), 0),
    }


def relative_index(span):
    coords = np.stack(np.meshgrid(np.arange(span), np.arange(span), np.arange(span), indexing='ij'), -1).reshape(-1, 3)
    offset = coords[:, None, :] - coords[None, :, :] + span - 1
    width = 2 * span - 1
    return (offset[..., 0] * width * width + offset[..., 1] * width + offset[..., 2]).reshape(-1).astype(np.int32)

def region_label(count):
    places = jnp.arange(count)
    return jnp.where(places < count - WIN, 0, jnp.where(places < count - SHIFT, 1, 2)).astype(jnp.int32)

def to_windows(array):
    first, second, third = array.shape[:3]
    rest = array.shape[3:]
    shaped = array.reshape((first // WIN, WIN, second // WIN, WIN, third // WIN, WIN) + rest)
    order = (0, 2, 4, 1, 3, 5) + tuple(range(6, 6 + len(rest)))
    return shaped.transpose(order).reshape((-1, WIN ** 3) + rest)

def from_windows(array, first, second, third):
    feats = array.shape[-1]
    shaped = array.reshape(first // WIN, second // WIN, third // WIN, WIN, WIN, WIN, feats)
    return shaped.transpose(0, 3, 1, 4, 2, 5, 6).reshape(first, second, third, feats)

def window_pass(ln_w, dy_w, lab_w, w_qkv, b_qkv, w_proj, bias_full):
    f32 = jnp.float32
    bf16 = jnp.bfloat16
    group, tok, feats = ln_w.shape
    heads = bias_full.shape[0]
    hdim = feats // heads
    scale = hdim ** (-0.5)
    qkv = jnp.einsum('gtc,cf->gtf', ln_w.astype(f32), w_qkv.astype(f32)) + b_qkv
    qkv = qkv.astype(bf16).reshape(group, tok, 3, heads, hdim)
    query = qkv[:, :, 0].transpose(0, 2, 1, 3).astype(f32)
    keys = qkv[:, :, 1].transpose(0, 2, 1, 3).astype(f32)
    values = qkv[:, :, 2].transpose(0, 2, 1, 3).astype(f32)
    scores = jnp.einsum('ghid,ghjd->ghij', query, keys) * scale + bias_full[None]
    allowed = (lab_w[:, :, None] == lab_w[:, None, :])[:, None]
    scores = jnp.where(allowed, scores, f32(-1e+30))
    top = lax.optimization_barrier(jnp.max(scores, -1, keepdims=True))
    expo = jnp.exp(scores - top)
    probs = expo / lax.optimization_barrier(jnp.sum(expo, -1, keepdims=True))
    probs_b = probs.astype(bf16).astype(f32)
    attended = jnp.einsum('ghij,ghjd->ghid', probs_b, values)
    attended = attended.transpose(0, 2, 1, 3).reshape(group, tok, feats).astype(bf16).astype(f32)
    grad_att = jnp.einsum('gtc,fc->gtf', dy_w.astype(f32), w_proj.astype(f32)).astype(bf16).astype(f32)
    proj_part = jnp.einsum('gtf,gtc->fc', attended, dy_w.astype(f32))
    grad_heads = grad_att.reshape(group, tok, heads, hdim).transpose(0, 2, 1, 3)
    grad_probs = jnp.einsum('ghid,ghjd->ghij', grad_heads, values)
    grad_v = jnp.einsum('ghij,ghid->ghjd', probs_b, grad_heads)
    grad_scores = probs * (grad_probs - lax.optimization_barrier(jnp.sum(probs * grad_probs, -1, keepdims=True)))
    rel_part = lax.optimization_barrier(jnp.sum(grad_scores, 0))
    scores_b = grad_scores.astype(bf16).astype(f32)
    grad_q = jnp.einsum('ghij,ghjd->ghid', scores_b, keys) * scale
    grad_k = jnp.einsum('ghij,ghid->ghjd', scores_b, query) * scale
    grad_qkv = jnp.stack([grad_q, grad_k, grad_v], 1).transpose(0, 3, 1, 2, 4).reshape(group, tok, 3 * feats)
    bias_part = lax.optimization_barrier(jnp.sum(grad_qkv, (0, 1)))
    qkv_b = grad_qkv.astype(bf16).astype(f32)
    weight_part = jnp.einsum('gtc,gtf->cf', ln_w.astype(f32), qkv_b)
    grad_in = jnp.einsum('gtf,cf->gtc', qkv_b, w_qkv.astype(f32))
    return (grad_in, (weight_part, bias_part, proj_part, rel_part))

def reference(inputs, d_out, layer_norm_gain, layer_norm_bias, w_qkv, b_qkv, w_proj, rel_bias):
    f32 = jnp.float32
    tok = WIN ** 3
    feats = inputs.shape[-1]
    xf = inputs.astype(f32)
    centered_input = xf - lax.optimization_barrier(jnp.mean(xf, -1, keepdims=True))
    inverse_deviation = lax.rsqrt(lax.optimization_barrier(jnp.mean(centered_input * centered_input, -1, keepdims=True)) + 1e-05)
    normalized_input = centered_input * inverse_deviation
    normalized_tokens = (normalized_input * layer_norm_gain + layer_norm_bias).astype(jnp.bfloat16)
    moved = jnp.roll(normalized_tokens, (-SHIFT, -SHIFT, -SHIFT), (0, 1, 2))
    grad_moved = jnp.roll(d_out, (-SHIFT, -SHIFT, -SHIFT), (0, 1, 2))
    labels = region_label(NX)[:, None, None] * 9 + region_label(NY)[None, :, None] * 3 + region_label(NZ)[None, None, :]
    index = jnp.asarray(relative_index(WIN)).astype(jnp.int32)
    bias_full = jnp.take(rel_bias, index, axis=1).reshape(HEADS, tok, tok)
    group = NZ // WIN
    win_ln = to_windows(moved).reshape(-1, group, tok, feats)
    win_dy = to_windows(grad_moved).reshape(-1, group, tok, feats)
    win_lab = to_windows(labels).reshape(-1, group, tok)

    def step(carry, item):
        grad_in, parts = window_pass(item[0], item[1], item[2], w_qkv, b_qkv, w_proj, bias_full)
        return (tuple((total + part for total, part in zip(carry, parts))), grad_in)
    start = (jnp.zeros((feats, 3 * feats), f32), jnp.zeros((3 * feats,), f32), jnp.zeros((feats, feats), f32), jnp.zeros((HEADS, tok, tok), f32))
    sums, grad_win = lax.scan(step, start, (win_ln, win_dy, win_lab))
    grad_in = from_windows(grad_win.reshape(-1, tok, feats), NX, NY, NZ)
    normalized_output_gradient = jnp.roll(grad_in, (SHIFT, SHIFT, SHIFT), (0, 1, 2))
    normalized_gradient = normalized_output_gradient * layer_norm_gain
    input_gradient_norm = inverse_deviation * (normalized_gradient - lax.optimization_barrier(jnp.mean(normalized_gradient, -1, keepdims=True)) - normalized_input * lax.optimization_barrier(jnp.mean(normalized_gradient * normalized_input, -1, keepdims=True)))
    d_x = (d_out.astype(f32) + input_gradient_norm).astype(jnp.bfloat16)
    rel_sum = jax.ops.segment_sum(sums[3].reshape(HEADS, -1).T, index, num_segments=TABLE).T
    inverse_width_factor = float(TOKENS) ** (-0.5)
    gain_gradient = lax.optimization_barrier(jnp.sum(normalized_output_gradient * normalized_input, (0, 1, 2))) * inverse_width_factor
    g_shift = lax.optimization_barrier(jnp.sum(normalized_output_gradient, (0, 1, 2))) * inverse_width_factor
    return (d_x, sums[0] * inverse_width_factor, sums[1] * inverse_width_factor, sums[2] * inverse_width_factor, rel_sum * inverse_width_factor, gain_gradient, g_shift)
```

```python
import functools

import jax
import jax.numpy as jnp
from jax import lax
from jax.experimental import pallas as pl
from jax.experimental.pallas import tpu as pltpu
from jax.sharding import PartitionSpec as P

WIN = 7
SHIFT = 3
TOK = WIN**3
ROWS = 344
LANES = 384
SLAB = 8 * WIN * WIN
SPAN = 2 * WIN - 1
WIDE = 1152
TABLE = 2304
HID = 112
AUG = 80
BIG = 1e30
F32 = jnp.float32
BF16 = jnp.bfloat16
NN = (((1,), (0,)), ((), ()))
NT = (((1,), (1,)), ((), ()))


def dot(left, right, dims=NN):
    return lax.dot_general(left, right, dims, preferred_element_type=F32)


def halves(value):
    high = value.astype(BF16)
    return high, (value - high.astype(F32)).astype(BF16)


def thirds(value):
    high = value.astype(BF16)
    rest = value - high.astype(F32)
    mid = rest.astype(BF16)
    return high, mid, (rest - mid.astype(F32)).astype(BF16)


def seventh(count):
    return (count * 9363) >> 16


def places(token):
    upper = seventh(token)
    first = seventh(upper)
    return first, upper - WIN * first, token - WIN * upper


def spread_ones():
    token = lax.broadcasted_iota(jnp.int32, (1, LANES), 1)
    first, second, third = places(token)
    target = jnp.where(token < TOK, first * SPAN * SPAN + second * SPAN + third, -1)
    row = lax.broadcasted_iota(jnp.int32, (WIDE, LANES), 0)
    return jnp.where(row == target, 1.0, 0.0).astype(BF16)


def shear(rows, sign):
    steps = WIN - 1 - lax.broadcasted_iota(jnp.int32, rows.shape, 0)
    for bit in (1, 2, 4):
        moved = pltpu.roll(rows, bit if sign > 0 else TABLE - bit, 1)
        rows = jnp.where((steps & bit) != 0, moved, rows)
    return rows


def offset_of(first, second):
    return (WIN - 1 - first) * SPAN * SPAN + (WIN - 1 - second) * SPAN


def expand_body(table_ref, bias_ref, base_ref, ones_ref, wide_ref):
    ones_ref[...] = spread_ones()
    heads = bias_ref.shape[0]
    for head in range(heads):
        row = jnp.broadcast_to(table_ref[head : head + 1, :], (8, TABLE))
        base_ref[...] = shear(row, -1)
        for first in range(WIN):
            for second in range(WIN):
                at = offset_of(first, second)
                rows = 8 * (first * WIN + second)
                wide_ref[rows : rows + 8, :] = base_ref[:, at : at + WIDE]
        high, mid, low = thirds(wide_ref[...])
        full = (dot(high, ones_ref[...]) + dot(mid, ones_ref[...])) + dot(low, ones_ref[...])
        for group in range(WIN * WIN):
            bias_ref[head, WIN * group : WIN * group + WIN, :] = full[8 * group : 8 * group + WIN]
        bias_ref[head, TOK:ROWS, :] = jnp.zeros((ROWS - TOK, LANES), F32)


def expand_table(table, heads, interpret=False):
    return pl.pallas_call(
        expand_body,
        out_shape=jax.ShapeDtypeStruct((heads, ROWS, LANES), F32),
        scratch_shapes=[
            pltpu.VMEM((8, TABLE), F32),
            pltpu.VMEM((WIDE, LANES), BF16),
            pltpu.VMEM((SLAB, WIDE), F32),
        ],
        cost_estimate=pl.CostEstimate(flops=9_000_000_000, bytes_accessed=2_000_000, transcendentals=0),
        interpret=interpret,
        name="expand",
    )(table)


def fold_body(pairs_ref, table_ref, rows_ref, ones_ref, total_ref):
    ones_ref[...] = spread_ones()
    heads = pairs_ref.shape[0]
    table_ref[...] = jnp.zeros(table_ref.shape, F32)
    rows_ref[...] = jnp.zeros(rows_ref.shape, F32)
    for head in range(heads):
        for group in range(WIN * WIN):
            rows_ref[8 * group : 8 * group + WIN, :] = pairs_ref[head, WIN * group : WIN * group + WIN, :]
        high, low = halves(rows_ref[...])
        wide = dot(high, ones_ref[...], NT) + dot(low, ones_ref[...], NT)
        total_ref[...] = jnp.zeros(total_ref.shape, F32)
        for first in range(WIN):
            for second in range(WIN):
                at = offset_of(first, second)
                rows = 8 * (first * WIN + second)
                total_ref[:, at : at + WIDE] = total_ref[:, at : at + WIDE] + wide[rows : rows + 8]
        sheared = shear(total_ref[...], 1)
        table_ref[head : head + 1, :] = jnp.sum(sheared, 0, keepdims=True)


def fold_table(pairs, interpret=False):
    return pl.pallas_call(
        fold_body,
        out_shape=jax.ShapeDtypeStruct((8, TABLE), F32),
        scratch_shapes=[
            pltpu.VMEM((SLAB, LANES), F32),
            pltpu.VMEM((WIDE, LANES), BF16),
            pltpu.VMEM((8, TABLE), F32),
        ],
        interpret=interpret,
        name="fold",
    )(pairs)


def window_body(
    flag_ref, xd_ref, bias_ref, gain_ref, shift_ref, wside_ref, wtrans_ref, wproj_ref, wq_ref, wkv_ref,
    dx_ref, pair_ref, gq_ref, gkv_ref, gproj_ref, vec_ref,
    pack_ref, unpack_ref, kmask_ref, qmask_ref, score_ref, expo_ref, grad_ref, qdiag_ref, odiag_ref,
    kaug_ref, vaug_ref, attn_ref, dq_ref,
):
    heads = pair_ref.shape[0]
    feats = wproj_ref.shape[0]
    hdim = feats // heads
    scale = hdim ** (-0.5)
    at = [pl.program_id(axis) for axis in range(3)]
    first_step = (at[0] == 0) & (at[1] == 0) & (at[2] == 0)

    @pl.when(first_step)
    def _():
        place = lax.broadcasted_iota(jnp.int32, (LANES, SLAB), 1)
        token = lax.broadcasted_iota(jnp.int32, (LANES, SLAB), 0)
        target = jnp.where((place & 7) == 7, -1, place - (place >> 3))
        pack_ref[...] = jnp.where(token == target, 1.0, 0.0).astype(BF16)
        place = lax.broadcasted_iota(jnp.int32, (SLAB, LANES), 0)
        token = lax.broadcasted_iota(jnp.int32, (SLAB, LANES), 1)
        target = jnp.where((place & 7) == 7, -1, place - (place >> 3))
        unpack_ref[...] = jnp.where(token == target, 1.0, 0.0).astype(BF16)
        row = lax.broadcasted_iota(jnp.int32, (ROWS, 128), 0)
        lane = lax.broadcasted_iota(jnp.int32, (ROWS, 128), 1)
        late = [(part >= WIN - SHIFT).astype(F32) for part in places(row)]
        value = jnp.zeros((ROWS, 128), F32)
        for axis in range(3):
            value = jnp.where(lane == 64 + 2 * axis, -BIG * (1.0 - late[axis]), value)
            value = jnp.where(lane == 65 + 2 * axis, -BIG * late[axis], value)
        value = jnp.where((lane == 70) & (row >= TOK), -BIG, value)
        kmask_ref[...] = value
        row = lax.broadcasted_iota(jnp.int32, (16, LANES), 0)
        lane = lax.broadcasted_iota(jnp.int32, (16, LANES), 1)
        late = [(part >= WIN - SHIFT).astype(F32) for part in places(lane)]
        value = jnp.where(row == 6, 1.0, 0.0)
        for axis in range(3):
            value = jnp.where(row == 2 * axis, late[axis], value)
            value = jnp.where(row == 2 * axis + 1, 1.0 - late[axis], value)
        qmask_ref[...] = value.astype(BF16)
        for ref in (pair_ref, gq_ref, gkv_ref, gproj_ref, vec_ref, qdiag_ref, odiag_ref):
            ref[...] = jnp.zeros(ref.shape, ref.dtype)

    block = xd_ref[...].astype(F32).reshape(SLAB, 256).astype(BF16)
    packed = dot(pack_ref[...], block)
    dy_tok = packed[:, 128:].astype(BF16)
    x_t = packed[:, :128].T[:feats]
    dy_t = packed[:, 128:].T[:feats]
    mu = jnp.sum(x_t, 0, keepdims=True) * (1.0 / feats)
    centered = x_t - mu
    rstd = lax.rsqrt(jnp.sum(centered * centered, 0, keepdims=True) * (1.0 / feats) + 1e-05)
    xhat = centered * rstd
    valid = (lax.broadcasted_iota(jnp.int32, (1, LANES), 1) < TOK).astype(F32)
    normed = (xhat * gain_ref[...] + shift_ref[...]) * valid
    row = lax.broadcasted_iota(jnp.int32, (128 - feats, LANES), 0)
    tail = jnp.where(row < 3, valid, 0.0)
    norm_full = jnp.concatenate([normed, tail], 0)
    norm_t = norm_full[:HID].astype(BF16)
    norm_tok = norm_full.T[:ROWS].astype(BF16)

    lane = lax.broadcasted_iota(jnp.int32, (1, 128), 1)
    flags = jnp.where(lane == 70, 1.0, 0.0)
    for axis in range(3):
        last = (at[axis] == pl.num_programs(axis) - 1).astype(F32) * flag_ref[axis]
        flags = jnp.where((lane == 64 + 2 * axis) | (lane == 65 + 2 * axis), last, flags)
    kmask = kmask_ref[...] * flags
    ones = jnp.where((lane >= 64) & (lane < 67), 1.0, 0.0)
    side = dot(norm_tok, wside_ref[...])
    for head in range(heads):
        kaug_ref[head] = (side[:, 128 * head : 128 * head + 128] + kmask).astype(BF16)
        base = 128 * (heads + head)
        vaug_ref[head] = (side[:, base : base + 128] + ones).astype(BF16)
    turned = dot(wtrans_ref[...], norm_t)
    q_at = 48 * heads
    k_at = q_at + feats
    q_t = turned[q_at : q_at + feats].astype(BF16)
    k_t = turned[k_at : k_at + feats].astype(BF16)
    do_t = dot(wproj_ref[...], dy_tok[:, :feats], NT).astype(BF16).astype(F32)
    scaled = q_t.astype(F32) * (scale * 1.4426950408889634)

    for head in range(heads):
        lo, hi = hdim * head, hdim * (head + 1)
        span = slice(LANES * head, LANES * (head + 1))
        q_high, q_low = halves(scaled[lo:hi])
        q_aug = jnp.concatenate([q_high, q_low, qmask_ref[...]], 0)
        score = dot(kaug_ref[head, :, :AUG], q_aug) + bias_ref[head]
        score_ref[...] = score
        top = jnp.max(score, 0, keepdims=True)
        expo = jnp.exp2(score_ref[...] - top).astype(BF16)
        expo_ref[:, span] = expo
        v_t = turned[48 * head : 48 * head + 48].astype(BF16)
        out = dot(v_t[:, :ROWS], expo_ref[:, span])
        inverse = 1.0 / out[hdim : hdim + 1]
        out = out[:hdim] * inverse
        attn_ref[lo:hi, :] = out.astype(BF16)
        grad_out = do_t[lo:hi]
        mean = jnp.sum(out * grad_out, 0, keepdims=True) * (-inverse)
        o_high, o_low = halves(grad_out * inverse)
        m_high, m_mid, m_low = thirds(mean)
        row16 = lax.broadcasted_iota(jnp.int32, (16, LANES), 0)
        m_rows = jnp.where(
            row16 == 0,
            m_high.astype(F32),
            jnp.where(row16 == 1, m_mid.astype(F32), jnp.where(row16 == 2, m_low.astype(F32), 0.0)),
        ).astype(BF16)
        o_aug = jnp.concatenate([o_high, o_low, m_rows], 0)
        grads = dot(vaug_ref[head, :, :AUG], o_aug) * expo_ref[:, span].astype(F32)
        pair_ref[head] = pair_ref[head] + grads
        grad_ref[:, span] = grads.astype(BF16)
        qdiag_ref[lo:hi, span] = q_t[lo:hi]
        odiag_ref[lo:hi, span] = o_high
        dq_ref[lo:hi, :] = (dot(k_t[lo:hi, :ROWS], grad_ref[:, span]) * scale).astype(BF16)

    dk = (dot(grad_ref[...], qdiag_ref[...], NT) * scale).astype(BF16)
    dv = dot(expo_ref[...], odiag_ref[...], NT).astype(BF16)
    dkv = jnp.concatenate([dk, dv], 1)
    dq = dq_ref[...]
    gq_ref[...] = gq_ref[...] + dot(norm_t, dq, NT)
    gkv_ref[...] = gkv_ref[...] + dot(norm_t[:, :ROWS], dkv)
    gproj_ref[...] = gproj_ref[...] + dot(attn_ref[...], dy_tok[:, :feats])
    dkv_all = jnp.concatenate([dkv, jnp.zeros((LANES - ROWS, 2 * feats), BF16)], 0)
    grad_in = dot(wq_ref[...], dq) + dot(wkv_ref[...], dkv_all, NT)
    vec_ref[0] = vec_ref[0] + grad_in * xhat
    vec_ref[1] = vec_ref[1] + grad_in
    dhat = grad_in * gain_ref[...]
    mean_one = jnp.sum(dhat, 0, keepdims=True) * (1.0 / feats)
    mean_two = jnp.sum(dhat * xhat, 0, keepdims=True) * (1.0 / feats)
    d_x = (dy_t + rstd * (dhat - mean_one - xhat * mean_two)).astype(BF16)
    spread = dot(unpack_ref[...], d_x, NT)
    dx_ref[...] = spread.reshape(WIN, WIN, 8, feats).astype(BF16)


def window_call(flags, xd, bias, gain, shift, wside, wtrans, wproj, wq, wkv, heads, interpret=False):
    feats = wproj.shape[0]
    grid = (xd.shape[0] // WIN, xd.shape[1] // WIN, xd.shape[2] // 8)

    def whole(array):
        zeros = (0,) * array.ndim
        return pl.BlockSpec(array.shape, lambda *_: zeros)

    def total(shape):
        zeros = (0,) * len(shape)
        return pl.BlockSpec(shape, lambda *_: zeros), jax.ShapeDtypeStruct(shape, F32)

    def tile(width):
        return pl.BlockSpec((WIN, WIN, 8, width), lambda i, j, k: (i, j, k, 0))

    sums = [
        total((heads, ROWS, LANES)),
        total((HID, feats)),
        total((HID, 2 * feats)),
        total((feats, feats)),
        total((2, feats, LANES)),
    ]
    return pl.pallas_call(
        window_body,
        grid=grid,
        in_specs=[pl.BlockSpec(memory_space=pltpu.SMEM), tile(256)]
        + [whole(a) for a in (bias, gain, shift, wside, wtrans, wproj, wq, wkv)],
        out_specs=[tile(feats)] + [s[0] for s in sums],
        out_shape=[jax.ShapeDtypeStruct(xd.shape[:3] + (feats,), BF16)] + [s[1] for s in sums],
        scratch_shapes=[
            pltpu.VMEM((LANES, SLAB), BF16),
            pltpu.VMEM((SLAB, LANES), BF16),
            pltpu.VMEM((ROWS, 128), F32),
            pltpu.VMEM((16, LANES), BF16),
            pltpu.VMEM((ROWS, LANES), F32),
            pltpu.VMEM((ROWS, heads * LANES), BF16),
            pltpu.VMEM((ROWS, heads * LANES), BF16),
            pltpu.VMEM((feats, heads * LANES), BF16),
            pltpu.VMEM((feats, heads * LANES), BF16),
            pltpu.VMEM((heads, ROWS, 128), BF16),
            pltpu.VMEM((heads, ROWS, 128), BF16),
            pltpu.VMEM((feats, LANES), BF16),
            pltpu.VMEM((feats, LANES), BF16),
        ],
        compiler_params=pltpu.CompilerParams(
            dimension_semantics=("arbitrary",) * 3, vmem_limit_bytes=60 * 1024 * 1024
        ),
        interpret=interpret,
        name="windows",
    )(flags, xd, bias, gain, shift, wside, wtrans, wproj, wq, wkv)


def side_weights(w_qkv, b_qkv, heads):
    feats = w_qkv.shape[0]
    hdim = feats // heads
    parts = thirds(b_qkv)
    full = jnp.concatenate(
        [w_qkv] + [p[None] for p in parts] + [jnp.zeros((128 - feats - 3, 3 * feats), BF16)], 0
    )
    cols = full.reshape(128, 3, heads, hdim)
    pad = jnp.zeros((128, 2, heads, 128 - 2 * hdim), BF16)
    wside = jnp.concatenate([cols[:, 1:], cols[:, 1:], pad], -1).reshape(128, 2 * heads * 128)
    v_rows = cols[:HID, 2].transpose(1, 2, 0)
    one = (jnp.arange(HID)[None, None, :] == feats) & (jnp.arange(16)[None, :, None] == 0)
    one = jnp.broadcast_to(one.astype(BF16), (heads, 16, HID))
    v_rows = jnp.concatenate([v_rows, one], 1).reshape(48 * heads, HID)
    qk_rows = full[:HID, : 2 * feats].T
    return wside, jnp.concatenate([v_rows, qk_rows], 0)


def shifted(block, axis, distance):
    devices = range(lax.axis_size(axis))
    route = [((i - distance) % len(devices), i) for i in devices]
    return lax.ppermute(block, axis, route)


def forward(field, dim, axis):
    arrived = shifted(lax.slice_in_dim(field, 0, SHIFT, axis=dim), axis, -1)
    return jnp.concatenate([lax.slice_in_dim(field, SHIFT, None, axis=dim), arrived], dim)


def backward(field, dim, axis):
    edge = field.shape[dim] - SHIFT
    arrived = shifted(lax.slice_in_dim(field, edge, None, axis=dim), axis, 1)
    return jnp.concatenate([arrived, lax.slice_in_dim(field, 0, edge, axis=dim)], dim)


def shards(inputs, d_out, layer_norm_gain, layer_norm_bias, w_qkv, b_qkv, w_proj, rel_bias):
    cells_x, cells_y, cells_z, feats = inputs.shape
    heads = rel_bias.shape[0]
    pad = jnp.zeros(inputs.shape[:3] + (128 - feats,), BF16)
    xd = jnp.concatenate([inputs, pad, d_out, pad], -1)
    for dim, axis in enumerate(("gx", "gy", "gz")):
        xd = forward(xd, dim, axis)
    deep = cells_z // WIN
    xd = xd.reshape(cells_x, cells_y, deep, WIN, 256)
    xd = jnp.pad(xd, ((0, 0), (0, 0), (0, 0), (0, 1), (0, 0))).reshape(cells_x, cells_y, deep * 8, 256)
    table = jnp.pad(rel_bias * 1.4426950408889634, ((0, 8 - heads), (0, TABLE - rel_bias.shape[1])))
    bias = expand_table(table, heads)
    wside, wtrans = side_weights(w_qkv, b_qkv, heads)
    gain = jnp.broadcast_to(layer_norm_gain[:, None], (feats, LANES))
    shift = jnp.broadcast_to(layer_norm_bias[:, None], (feats, LANES))
    flags = jnp.stack(
        [(lax.axis_index(a) == lax.axis_size(a) - 1).astype(F32) for a in ("gx", "gy", "gz")]
    )
    d_x, pairs, gq, gkv, gproj, vec = window_call(
        flags, xd, bias, gain, shift, wside, wtrans, w_proj, w_qkv[:, :feats], w_qkv[:, feats:], heads
    )
    d_x = d_x.reshape(cells_x, cells_y, deep, 8, feats)[:, :, :, :WIN].reshape(inputs.shape)
    for dim, axis in enumerate(("gx", "gy", "gz")):
        d_x = backward(d_x, dim, axis)
    rel = fold_table(pairs)[:heads]
    vec = jnp.sum(vec, -1)
    both = jnp.concatenate([gq, gkv], 1)
    count = inputs.shape[0] * inputs.shape[1] * inputs.shape[2]
    for a in ("gx", "gy", "gz"):
        count *= lax.axis_size(a)
    totals = lax.psum((both, gproj, rel, vec), ("gx", "gy", "gz"))
    both, gproj, rel, vec = [t * float(count) ** (-0.5) for t in totals]
    return (
        d_x, both[:feats], both[feats], gproj, rel[:, : rel_bias.shape[1]], vec[0], vec[1],
    )


def solution(mesh):
    placed = (P("gx", "gy", "gz", None), P("gx", "gy", "gz", None), P(), P(), P(), P(), P(), P())
    return jax.shard_map(
        shards,
        mesh=mesh,
        in_specs=placed,
        out_specs=(P("gx", "gy", "gz", None), P(), P(), P(), P(), P(), P()),
        check_vma=False,
    )
```

```python
import functools

import jax
import jax.numpy as jnp
from jax import lax
from jax.experimental import pallas as pl
from jax.experimental.pallas import tpu as pltpu
from jax.sharding import PartitionSpec as P

WIN = 7
SHIFT = 3
TOK = WIN**3
ROWS = 344
LANES = 384
SLAB = 8 * WIN * WIN
SPAN = 2 * WIN - 1
WIDE = 1152
TABLE = 2304
HID = 112
REL_AT = 104
AUG = 80
BIG = 1e30
F32 = jnp.float32
BF16 = jnp.bfloat16
NN = (((1,), (0,)), ((), ()))
NT = (((1,), (1,)), ((), ()))


def dot(left, right, dims=NN):
    return lax.dot_general(left, right, dims, preferred_element_type=F32)


def halves(value):
    high = value.astype(BF16)
    return high, (value - high.astype(F32)).astype(BF16)


def thirds(value):
    high = value.astype(BF16)
    rest = value - high.astype(F32)
    mid = rest.astype(BF16)
    return high, mid, (rest - mid.astype(F32)).astype(BF16)


def seventh(count):
    return (count * 9363) >> 16


def places(token):
    upper = seventh(token)
    first = seventh(upper)
    return first, upper - WIN * first, token - WIN * upper


def spread_ones():
    token = lax.broadcasted_iota(jnp.int32, (1, LANES), 1)
    first, second, third = places(token)
    target = jnp.where(token < TOK, first * SPAN * SPAN + second * SPAN + third, -1)
    row = lax.broadcasted_iota(jnp.int32, (WIDE, LANES), 0)
    return jnp.where(row == target, 1.0, 0.0).astype(BF16)


def shear(rows, sign):
    steps = WIN - 1 - lax.broadcasted_iota(jnp.int32, rows.shape, 0)
    for bit in (1, 2, 4):
        moved = pltpu.roll(rows, bit if sign > 0 else TABLE - bit, 1)
        rows = jnp.where((steps & bit) != 0, moved, rows)
    return rows


def offset_of(first, second):
    return (WIN - 1 - first) * SPAN * SPAN + (WIN - 1 - second) * SPAN


def slab_token(place):
    third = place & 7
    third = third + (WIN - SHIFT) - jnp.where(third >= SHIFT, WIN, 0)
    return jnp.where((place & 7) == 7, -1, (place >> 3) * WIN + third)


def expand_body(table_ref, bias_ref, pack_ref, unpack_ref, kmask_ref, qmask_ref, base_ref, ones_ref, wide_ref):
    place = lax.broadcasted_iota(jnp.int32, (LANES, SLAB), 1)
    token = lax.broadcasted_iota(jnp.int32, (LANES, SLAB), 0)
    pack_ref[...] = jnp.where(token == slab_token(place), 1.0, 0.0).astype(BF16)
    place = lax.broadcasted_iota(jnp.int32, (SLAB, LANES), 0)
    token = lax.broadcasted_iota(jnp.int32, (SLAB, LANES), 1)
    unpack_ref[...] = jnp.where(token == slab_token(place), 1.0, 0.0).astype(BF16)
    row = lax.broadcasted_iota(jnp.int32, (ROWS, 128), 0)
    lane = lax.broadcasted_iota(jnp.int32, (ROWS, 128), 1)
    late = [(part >= WIN - SHIFT).astype(F32) for part in places(row)]
    value = jnp.zeros((ROWS, 128), F32)
    for axis in range(3):
        value = jnp.where(lane == 64 + 2 * axis, -BIG * (1.0 - late[axis]), value)
        value = jnp.where(lane == 65 + 2 * axis, -BIG * late[axis], value)
    value = jnp.where((lane == 70) & (row >= TOK), -BIG, value)
    kmask_ref[...] = value
    row = lax.broadcasted_iota(jnp.int32, (16, LANES), 0)
    lane = lax.broadcasted_iota(jnp.int32, (16, LANES), 1)
    late = [(part >= WIN - SHIFT).astype(F32) for part in places(lane)]
    value = jnp.where(row == 6, 1.0, 0.0)
    for axis in range(3):
        value = jnp.where(row == 2 * axis, late[axis], value)
        value = jnp.where(row == 2 * axis + 1, 1.0 - late[axis], value)
    qmask_ref[...] = value.astype(BF16)
    ones_ref[...] = spread_ones()
    heads = bias_ref.shape[0]
    for head in range(heads):
        row = jnp.broadcast_to(table_ref[head : head + 1, :], (8, TABLE))
        base_ref[...] = shear(row, -1)
        for first in range(WIN):
            for second in range(WIN):
                at = offset_of(first, second)
                rows = 8 * (first * WIN + second)
                wide_ref[rows : rows + 8, :] = base_ref[:, at : at + WIDE]
        high, mid, low = thirds(wide_ref[...])
        full = (dot(high, ones_ref[...]) + dot(mid, ones_ref[...])) + dot(low, ones_ref[...])
        for group in range(WIN * WIN):
            bias_ref[head, WIN * group : WIN * group + WIN, :] = full[8 * group : 8 * group + WIN]
        bias_ref[head, TOK:ROWS, :] = jnp.zeros((ROWS - TOK, LANES), F32)


def expand_table(table, heads, interpret=False):
    return pl.pallas_call(
        expand_body,
        out_shape=[
            jax.ShapeDtypeStruct((heads, ROWS, LANES), F32),
            jax.ShapeDtypeStruct((LANES, SLAB), BF16),
            jax.ShapeDtypeStruct((SLAB, LANES), BF16),
            jax.ShapeDtypeStruct((ROWS, 128), F32),
            jax.ShapeDtypeStruct((16, LANES), BF16),
        ],
        scratch_shapes=[
            pltpu.VMEM((8, TABLE), F32),
            pltpu.VMEM((WIDE, LANES), BF16),
            pltpu.VMEM((SLAB, WIDE), F32),
        ],
        cost_estimate=pl.CostEstimate(flops=4_000_000_000, bytes_accessed=2_000_000, transcendentals=0),
        interpret=interpret,
        name="expand",
    )(table)


def column_sums(value):
    part = value[:, :128] + value[:, 128:256] + value[:, 256:]
    part = jnp.concatenate([part, jnp.zeros((128 - part.shape[0], 128), F32)], 0)
    return jnp.sum(part.T, 0, keepdims=True)


def fold_body(pairs_ref, gq_ref, gkv_ref, gproj_ref, vec_ref, out_ref, rows_ref, ones_ref, total_ref):
    ones_ref[...] = spread_ones()
    heads = pairs_ref.shape[0]
    feats = gproj_ref.shape[0]
    out_ref[...] = jnp.zeros(out_ref.shape, F32)
    proj = jnp.concatenate([gproj_ref[...], jnp.zeros((8, feats), F32)], 0)
    out_ref[:REL_AT, :] = jnp.concatenate([gq_ref[:REL_AT], gkv_ref[:REL_AT], proj], 1)
    for at in range(2):
        out_ref[feats + 1 + at : feats + 2 + at, :128] = column_sums(vec_ref[at])
    rows_ref[...] = jnp.zeros(rows_ref.shape, F32)
    for head in range(heads):
        for group in range(WIN * WIN):
            rows_ref[8 * group : 8 * group + WIN, :] = pairs_ref[head, WIN * group : WIN * group + WIN, :]
        high, low = halves(rows_ref[...])
        wide = dot(high, ones_ref[...], NT) + dot(low, ones_ref[...], NT)
        total_ref[...] = jnp.zeros(total_ref.shape, F32)
        for first in range(WIN):
            for second in range(WIN):
                at = offset_of(first, second)
                rows = 8 * (first * WIN + second)
                total_ref[:, at : at + WIDE] = total_ref[:, at : at + WIDE] + wide[rows : rows + 8]
        entries = jnp.sum(shear(total_ref[...], 1), 0, keepdims=True)
        for part in range(TABLE // LANES):
            row = REL_AT + head * (TABLE // LANES) + part
            out_ref[row : row + 1, :] = entries[:, LANES * part : LANES * part + LANES]


def fold_sums(sums, interpret=False):
    return pl.pallas_call(
        fold_body,
        out_shape=jax.ShapeDtypeStruct((128, LANES), F32),
        scratch_shapes=[
            pltpu.VMEM((SLAB, LANES), F32),
            pltpu.VMEM((WIDE, LANES), BF16),
            pltpu.VMEM((8, TABLE), F32),
        ],
        cost_estimate=pl.CostEstimate(flops=3_000_000_000, bytes_accessed=2_000_000, transcendentals=0),
        interpret=interpret,
        name="fold",
    )(*sums)


def gather(x_ref, d_ref, yhalo_ref, xhalo_ref, zhalo_ref, block_ref, base, last):
    feats = x_ref.shape[3]
    row, col = pl.program_id(0), pl.program_id(1)
    at_x = WIN * (row + base) + SHIFT
    at_y = WIN * col + SHIFT
    edge = WIN - SHIFT
    last_col = col == pl.num_programs(1) - 1

    def own(first, count_x, second, count_y):
        spot = (pl.ds(at_x + first, count_x), pl.ds(at_y + second, count_y))
        here = (slice(first, first + count_x), slice(second, second + count_y), slice(0, WIN))
        block_ref[here + (slice(0, feats),)] = x_ref[spot].astype(F32)
        block_ref[here + (slice(128, 128 + feats),)] = d_ref[spot].astype(F32)

    def arrived(first, count_x):
        block_ref[first : first + count_x, edge:, :WIN, :] = yhalo_ref[pl.ds(at_x + first, count_x)].astype(F32)

    def rows(first, count_x):
        own(first, count_x, 0, edge)

        @pl.when(last_col)
        def _():
            arrived(first, count_x)

        @pl.when(jnp.logical_not(last_col))
        def _():
            own(first, count_x, edge, SHIFT)

    if xhalo_ref is None:
        rows(0, WIN)
    else:
        last_row = row == pl.num_programs(0) - 1
        rows(0, edge)

        @pl.when(last_row)
        def _():
            block_ref[edge:, :, :WIN, :] = xhalo_ref[:, pl.ds(WIN * col, WIN)].astype(F32)

        @pl.when(jnp.logical_not(last_row))
        def _():
            rows(edge, SHIFT)

    block_ref[:, :, :SHIFT, :] = zhalo_ref[pl.ds(WIN * row, WIN), pl.ds(WIN * col, WIN)].astype(F32)


def window_body(base, has_xhalo, has_sums, *refs):
    refs = list(refs)
    flag_ref, x_ref, d_ref, yhalo_ref, zhalo_ref = refs[:5]
    refs = refs[5:]
    xhalo_ref = refs.pop(0) if has_xhalo else None
    bias_ref, pack_ref, unpack_ref, kmask_ref, qmask_ref = refs[:5]
    gain_ref, shift_ref, wside_ref, wtrans_ref, wproj_ref, wqkv_ref = refs[5:11]
    refs = refs[11:]
    before = [refs.pop(0) for _ in range(5)] if has_sums else None
    dx_ref, pair_ref, gq_ref, gkv_ref, gproj_ref, vec_ref = refs[:6]
    (block_ref, score_ref, expo_ref, grad_ref, qdiag_ref, odiag_ref, kaug_ref, vaug_ref, attn_ref, dq_ref) = refs[6:]
    sums = (pair_ref, gq_ref, gkv_ref, gproj_ref, vec_ref)
    heads = pair_ref.shape[0]
    feats = wproj_ref.shape[0]
    hdim = feats // heads
    scale = hdim ** (-0.5)
    row, col = pl.program_id(0), pl.program_id(1)
    last = [
        ((row == pl.num_programs(0) - 1) if has_xhalo else False),
        col == pl.num_programs(1) - 1,
        True,
    ]

    @pl.when((row == 0) & (col == 0))
    def _():
        for at, ref in enumerate(sums):
            ref[...] = jnp.zeros(ref.shape, ref.dtype) if before is None else before[at][...]
        for ref in (block_ref, qdiag_ref, odiag_ref):
            ref[...] = jnp.zeros(ref.shape, ref.dtype)

    gather(x_ref, d_ref, yhalo_ref, xhalo_ref, zhalo_ref, block_ref, base, last)
    block = block_ref[...].reshape(SLAB, 256).astype(BF16)
    packed = dot(pack_ref[...], block)
    dy_tok = packed[:, 128:].astype(BF16)
    x_t = packed[:, :128].T[:feats]
    dy_t = packed[:, 128:].T[:feats]
    mu = jnp.sum(x_t, 0, keepdims=True) * (1.0 / feats)
    centered = x_t - mu
    rstd = lax.rsqrt(jnp.sum(centered * centered, 0, keepdims=True) * (1.0 / feats) + 1e-05)
    xhat = centered * rstd
    valid = (lax.broadcasted_iota(jnp.int32, (1, LANES), 1) < TOK).astype(F32)
    normed = (xhat * gain_ref[...] + shift_ref[...]) * valid
    row = lax.broadcasted_iota(jnp.int32, (128 - feats, LANES), 0)
    tail = jnp.where(row < 3, valid, 0.0)
    norm_full = jnp.concatenate([normed, tail], 0)
    norm_t = norm_full[:HID].astype(BF16)
    norm_tok = norm_full.T[:ROWS].astype(BF16)

    lane = lax.broadcasted_iota(jnp.int32, (1, 128), 1)
    flags = jnp.where(lane == 70, 1.0, 0.0)
    for axis in range(3):
        edge = jnp.where(last[axis], flag_ref[axis], 0.0)
        flags = jnp.where((lane == 64 + 2 * axis) | (lane == 65 + 2 * axis), edge, flags)
    kmask = kmask_ref[...] * flags
    ones = jnp.where((lane >= 64) & (lane < 67), 1.0, 0.0)
    side = dot(norm_tok, wside_ref[...])
    for head in range(heads):
        kaug_ref[head] = (side[:, 128 * head : 128 * head + 128] + kmask).astype(BF16)
        base = 128 * (heads + head)
        vaug_ref[head] = (side[:, base : base + 128] + ones).astype(BF16)
    turned = dot(wtrans_ref[...], norm_t)
    q_at = 48 * heads
    k_at = q_at + feats
    q_t = turned[q_at : q_at + feats].astype(BF16)
    k_t = turned[k_at : k_at + feats].astype(BF16)
    do_t = dot(wproj_ref[...], dy_tok[:, :feats], NT).astype(BF16).astype(F32)
    scaled = q_t.astype(F32) * (scale * 1.4426950408889634)

    for head in range(heads):
        lo, hi = hdim * head, hdim * (head + 1)
        span = slice(LANES * head, LANES * (head + 1))
        q_high, q_low = halves(scaled[lo:hi])
        q_aug = jnp.concatenate([q_high, q_low, qmask_ref[...]], 0)
        score = dot(kaug_ref[head, :, :AUG], q_aug) + bias_ref[head]
        score_ref[...] = score
        top = jnp.max(score, 0, keepdims=True)
        expo = jnp.exp2(score_ref[...] - top).astype(BF16)
        expo_ref[:, span] = expo
        v_t = turned[48 * head : 48 * head + 48].astype(BF16)
        out = dot(v_t[:, :ROWS], expo_ref[:, span])
        inverse = 1.0 / out[hdim : hdim + 1]
        out = out[:hdim] * inverse
        attn_ref[lo:hi, :] = out.astype(BF16)
        grad_out = do_t[lo:hi]
        mean = jnp.sum(out * grad_out, 0, keepdims=True) * (-inverse)
        o_high, o_low = halves(grad_out * inverse)
        m_high, m_mid, m_low = thirds(mean)
        row16 = lax.broadcasted_iota(jnp.int32, (16, LANES), 0)
        m_rows = jnp.where(
            row16 == 0,
            m_high.astype(F32),
            jnp.where(row16 == 1, m_mid.astype(F32), jnp.where(row16 == 2, m_low.astype(F32), 0.0)),
        ).astype(BF16)
        o_aug = jnp.concatenate([o_high, o_low, m_rows], 0)
        grads = dot(vaug_ref[head, :, :AUG], o_aug) * expo_ref[:, span].astype(F32)
        pair_ref[head] = pair_ref[head] + grads
        grad_ref[:, span] = grads.astype(BF16)
        qdiag_ref[lo:hi, span] = q_t[lo:hi]
        odiag_ref[lo:hi, span] = o_high
        dq_ref[lo:hi, :] = (dot(k_t[lo:hi, :ROWS], grad_ref[:, span]) * scale).astype(BF16)

    dk = (dot(grad_ref[...], qdiag_ref[...], NT) * scale).astype(BF16)
    dv = dot(expo_ref[...], odiag_ref[...], NT).astype(BF16)
    dkv = jnp.concatenate([dk, dv], 1)
    dq = dq_ref[...]
    gq_ref[...] = gq_ref[...] + dot(norm_t, dq, NT)
    gkv_ref[...] = gkv_ref[...] + dot(norm_t[:, :ROWS], dkv)
    gproj_ref[...] = gproj_ref[...] + dot(attn_ref[...], dy_tok[:, :feats])
    dkv_all = jnp.concatenate([dkv, jnp.zeros((LANES - ROWS, 2 * feats), BF16)], 0)
    grad_in = dot(wqkv_ref[:, :feats], dq) + dot(wqkv_ref[:, feats:], dkv_all, NT)
    vec_ref[0] = vec_ref[0] + grad_in * xhat
    vec_ref[1] = vec_ref[1] + grad_in
    dhat = grad_in * gain_ref[...]
    mean_one = jnp.sum(dhat, 0, keepdims=True) * (1.0 / feats)
    mean_two = jnp.sum(dhat * xhat, 0, keepdims=True) * (1.0 / feats)
    d_x = (dy_t + rstd * (dhat - mean_one - xhat * mean_two)).astype(BF16)
    spread = dot(unpack_ref[...], d_x, NT)
    dx_ref[...] = spread.reshape(WIN, WIN, 8, feats).astype(BF16)


def window_call(base, count, flags, own, yhalo, zhalo, xhalo, tables, weights, sums, heads, interpret=False):
    cells_x, cells_y, cells_z, feats = own[0].shape
    grid = (count, cells_y // WIN)

    def whole(array):
        zeros = (0,) * array.ndim
        return pl.BlockSpec(array.shape, lambda *_: zeros)

    arrays = list(own) + [yhalo, zhalo] + ([] if xhalo is None else [xhalo])
    arrays += list(tables) + list(weights) + ([] if sums is None else list(sums))
    shapes = [(heads, ROWS, LANES), (HID, feats), (HID, 2 * feats), (feats, feats), (2, feats, LANES)]
    shapes = [jax.ShapeDtypeStruct(shape, F32) for shape in shapes]
    return pl.pallas_call(
        functools.partial(window_body, base, xhalo is not None, sums is not None),
        grid=grid,
        in_specs=[pl.BlockSpec(memory_space=pltpu.SMEM)] + [whole(a) for a in arrays],
        out_specs=[pl.BlockSpec((WIN, WIN, 8, feats), lambda i, j: (i, j, 0, 0))] + [whole(s) for s in shapes],
        out_shape=[jax.ShapeDtypeStruct((WIN * count, cells_y, 8, feats), BF16)] + shapes,
        scratch_shapes=[
            pltpu.VMEM((WIN, WIN, 8, 256), F32),
            pltpu.VMEM((ROWS, LANES), F32),
            pltpu.VMEM((ROWS, heads * LANES), BF16),
            pltpu.VMEM((ROWS, heads * LANES), BF16),
            pltpu.VMEM((feats, heads * LANES), BF16),
            pltpu.VMEM((feats, heads * LANES), BF16),
            pltpu.VMEM((heads, ROWS, 128), BF16),
            pltpu.VMEM((heads, ROWS, 128), BF16),
            pltpu.VMEM((feats, LANES), BF16),
            pltpu.VMEM((feats, LANES), BF16),
        ],
        compiler_params=pltpu.CompilerParams(
            dimension_semantics=("arbitrary",) * 2, vmem_limit_bytes=56 * 1024 * 1024
        ),
        cost_estimate=pl.CostEstimate(
            flops=2_200_000_000 * count * grid[1], bytes_accessed=8_000_000, transcendentals=0
        ),
        interpret=interpret,
        name="windows",
    )(flags, *arrays)


def side_weights(w_qkv, b_qkv, heads):
    feats = w_qkv.shape[0]
    hdim = feats // heads
    parts = thirds(b_qkv)
    full = jnp.concatenate(
        [w_qkv] + [p[None] for p in parts] + [jnp.zeros((128 - feats - 3, 3 * feats), BF16)], 0
    )
    cols = full.reshape(128, 3, heads, hdim)
    pad = jnp.zeros((128, 2, heads, 128 - 2 * hdim), BF16)
    wside = jnp.concatenate([cols[:, 1:], cols[:, 1:], pad], -1).reshape(128, 2 * heads * 128)
    v_rows = cols[:HID, 2].transpose(1, 2, 0)
    one = (jnp.arange(HID)[None, None, :] == feats) & (jnp.arange(16)[None, :, None] == 0)
    one = jnp.broadcast_to(one.astype(BF16), (heads, 16, HID))
    v_rows = jnp.concatenate([v_rows, one], 1).reshape(48 * heads, HID)
    qk_rows = full[:HID, : 2 * feats].T
    return wside, jnp.concatenate([v_rows, qk_rows], 0)


def shifted(block, axis, distance):
    count = lax.axis_size(axis)
    return lax.ppermute(block, axis, [((i - distance) % count, i) for i in range(count)])


def crossed(block, axis, bit):
    return lax.ppermute(block, axis, [(i, i ^ bit) for i in range(lax.axis_size(axis))])


def sum_everywhere(value, axes):
    sizes = {axis: lax.axis_size(axis) for axis in axes}
    if any(size & (size - 1) for size in sizes.values()) or sizes[axes[1]] < 2:
        return lax.psum(value, axes)
    near = axes[1]
    bit = lax.axis_index(near) & 1
    size = value.shape[0] // 2
    keep = lax.dynamic_slice_in_dim(value, bit * size, size, 0)
    send = lax.dynamic_slice_in_dim(value, (1 - bit) * size, size, 0)
    part = keep + crossed(send, near, 1)
    for axis in (axes[2], axes[1], axes[0]):
        step = 2 if axis == near else 1
        while step < sizes[axis]:
            part = part + crossed(part, axis, step)
            step *= 2
    other = crossed(part, near, 1)
    upper = bit == 1
    return jnp.concatenate([jnp.where(upper, other, part), jnp.where(upper, part, other)], 0)


def both(first, second):
    pad = jnp.zeros(first.shape[:3] + (128 - first.shape[3],), BF16)
    return jnp.concatenate([first, pad, second, pad], -1)


CHUNKS = (1, 3)


def shards(inputs, d_out, layer_norm_gain, layer_norm_bias, w_qkv, b_qkv, w_proj, rel_bias):
    cells_x, cells_y, cells_z, feats = inputs.shape
    heads = rel_bias.shape[0]
    axes = ("gx", "gy", "gz")
    rows = cells_x // WIN
    counts = [CHUNKS[0], rows - CHUNKS[0]] if rows > CHUNKS[0] else [rows]
    bases = [sum(counts[:i]) for i in range(len(counts))]

    def layers(lo, hi, depth):
        return jnp.concatenate(
            [both(inputs[lo:hi, SHIFT:, :depth], d_out[lo:hi, SHIFT:, :depth]), yhalo[lo:hi, :, :depth]], 1
        )

    yhalo = shifted(both(inputs[:, :SHIFT], d_out[:, :SHIFT]), "gy", -1)
    xhalo = shifted(layers(0, SHIFT, cells_z), "gx", -1)
    zhalos = []
    for base, count in zip(bases, counts):
        lo, hi = WIN * base + SHIFT, WIN * (base + count) + SHIFT
        edge = layers(lo, min(hi, cells_x), SHIFT)
        if hi > cells_x:
            edge = jnp.concatenate([edge, xhalo[:, :, :SHIFT]], 0)
        zhalos.append(shifted(edge, "gz", -1))
    table = jnp.pad(rel_bias * 1.4426950408889634, ((0, 8 - heads), (0, TABLE - rel_bias.shape[1])))
    tables = expand_table(table, heads)
    wside, wtrans = side_weights(w_qkv, b_qkv, heads)
    gain = jnp.broadcast_to(layer_norm_gain[:, None], (feats, LANES))
    shift = jnp.broadcast_to(layer_norm_bias[:, None], (feats, LANES))
    weights = (gain, shift, wside, wtrans, w_proj, w_qkv)
    flags = jnp.stack([(lax.axis_index(a) == lax.axis_size(a) - 1).astype(F32) for a in axes])
    sums, fields = None, []
    for at, (base, count) in enumerate(zip(bases, counts)):
        last = at == len(counts) - 1
        field, *sums = window_call(
            base, count, flags, (inputs, d_out), yhalo, zhalos[at], xhalo if last else None, tables, weights,
            sums, heads,
        )
        arrived = shifted(field[:, :, :SHIFT], "gz", 1)
        fields.append(jnp.concatenate([arrived, field[:, :, SHIFT:cells_z]], 2))
    total = sum_everywhere(fold_sums(sums), axes)
    arrived = shifted(fields[-1][-SHIFT:], "gx", 1)
    d_x = jnp.concatenate([arrived] + fields[:-1] + [fields[-1][:-SHIFT]], 0)
    edge = cells_y - SHIFT
    d_x = jnp.concatenate([shifted(d_x[:, edge:], "gy", 1), d_x[:, :edge]], 1)
    count = inputs.shape[0] * inputs.shape[1] * inputs.shape[2]
    for a in axes:
        count *= lax.axis_size(a)
    total = total * float(count) ** (-0.5)
    per_head = TABLE // LANES
    rel = total[REL_AT : REL_AT + heads * per_head].reshape(heads, TABLE)
    return (
        d_x,
        total[:feats, : 3 * feats],
        total[feats, : 3 * feats],
        total[:feats, 3 * feats :],
        rel[:, : rel_bias.shape[1]],
        total[feats + 1, :feats],
        total[feats + 2, :feats],
    )


def solution(mesh):
    placed = (P("gx", "gy", "gz", None), P("gx", "gy", "gz", None), P(), P(), P(), P(), P(), P())
    return jax.shard_map(
        shards,
        mesh=mesh,
        in_specs=placed,
        out_specs=(P("gx", "gy", "gz", None), P(), P(), P(), P(), P(), P()),
        check_vma=False,
    )
```

```python
import functools
import itertools

import jax
import jax.numpy as jnp
from jax import lax
from jax.experimental import pallas as pl
from jax.experimental.pallas import tpu as pltpu
from jax.sharding import PartitionSpec as P

WIN = 7
SHIFT = 3
TOK = WIN**3
ROWS = 344
LANES = 384
SLAB = 8 * WIN * WIN
SPAN = 2 * WIN - 1
WIDE = 1152
TABLE = 2304
HID = 112
AUG = 80
BIG = 1e30
F32 = jnp.float32
BF16 = jnp.bfloat16
NN = (((1,), (0,)), ((), ()))
NT = (((1,), (1,)), ((), ()))


def dot(left, right, dims=NN):
    return lax.dot_general(left, right, dims, preferred_element_type=F32)


def halves(value):
    high = value.astype(BF16)
    return high, (value - high.astype(F32)).astype(BF16)


def thirds(value):
    high = value.astype(BF16)
    rest = value - high.astype(F32)
    mid = rest.astype(BF16)
    return high, mid, (rest - mid.astype(F32)).astype(BF16)


def seventh(count):
    return (count * 9363) >> 16


def places(token):
    upper = seventh(token)
    first = seventh(upper)
    return first, upper - WIN * first, token - WIN * upper


def spread_ones():
    token = lax.broadcasted_iota(jnp.int32, (1, LANES), 1)
    first, second, third = places(token)
    target = jnp.where(token < TOK, first * SPAN * SPAN + second * SPAN + third, -1)
    row = lax.broadcasted_iota(jnp.int32, (WIDE, LANES), 0)
    return jnp.where(row == target, 1.0, 0.0).astype(BF16)


def shear(rows, sign):
    steps = WIN - 1 - lax.broadcasted_iota(jnp.int32, rows.shape, 0)
    for bit in (1, 2, 4):
        moved = pltpu.roll(rows, bit if sign > 0 else TABLE - bit, 1)
        rows = jnp.where((steps & bit) != 0, moved, rows)
    return rows


def offset_of(first, second):
    return (WIN - 1 - first) * SPAN * SPAN + (WIN - 1 - second) * SPAN


def slab_token(place):
    third = place & 7
    third = third + (WIN - SHIFT) - jnp.where(third >= SHIFT, WIN, 0)
    return jnp.where((place & 7) == 7, -1, (place >> 3) * WIN + third)


CUT, LOW, HIGH = 256, 896, 768


def weight_tables(wqkv_ref, bqkv_ref, wside_ref, wtrans_ref, heads):
    feats = wqkv_ref.shape[0]
    hdim = feats // heads
    rows = [part.astype(F32) for part in thirds(bqkv_ref[...])]
    full = jnp.concatenate(
        [wqkv_ref[...].astype(F32)] + rows + [jnp.zeros((128 - feats - 3, 3 * feats), F32)], 0
    )
    pad = jnp.zeros((128, 128 - 2 * hdim), F32)
    for part in range(2):
        for head in range(heads):
            lo = feats * (part + 1) + hdim * head
            piece = full[:, lo : lo + hdim]
            at = 128 * (part * heads + head)
            wside_ref[:, at : at + 128] = jnp.concatenate([piece, piece, pad], 1).astype(BF16)
    turned = jnp.concatenate([full, jnp.zeros((128, LANES - 3 * feats), F32)], 1).T[:, :HID]
    row = lax.broadcasted_iota(jnp.int32, (16, HID), 0)
    lane = lax.broadcasted_iota(jnp.int32, (16, HID), 1)
    one = jnp.where((row == 0) & (lane == feats), 1.0, 0.0).astype(BF16)
    for head in range(heads):
        lo = 2 * feats + hdim * head
        wtrans_ref[48 * head : 48 * head + hdim] = turned[lo : lo + hdim].astype(BF16)
        wtrans_ref[48 * head + hdim : 48 * head + 48] = one
    wtrans_ref[48 * heads :] = turned[: 2 * feats].astype(BF16)


def expand_body(
    table_ref, wqkv_ref, bqkv_ref, gain_ref, shift_ref,
    bias_ref, pack_ref, unpack_ref, kmask_ref, qmask_ref, wside_ref, wtrans_ref, gains_ref, shifts_ref,
    base_ref, ones_ref, wide_ref,
):
    weight_tables(wqkv_ref, bqkv_ref, wside_ref, wtrans_ref, bias_ref.shape[0])
    for source, target in ((gain_ref, gains_ref), (shift_ref, shifts_ref)):
        turned = jnp.broadcast_to(source[...], (128, source.shape[1]))
        turned = jnp.concatenate([turned, jnp.zeros((128, 128 - source.shape[1]), F32)], 1).T
        for part in range(LANES // 128):
            target[:, 128 * part : 128 * part + 128] = turned[: source.shape[1]]
    place = lax.broadcasted_iota(jnp.int32, (LANES, SLAB), 1)
    token = lax.broadcasted_iota(jnp.int32, (LANES, SLAB), 0)
    pack_ref[...] = jnp.where(token == slab_token(place), 1.0, 0.0).astype(BF16)
    place = lax.broadcasted_iota(jnp.int32, (SLAB, LANES), 0)
    token = lax.broadcasted_iota(jnp.int32, (SLAB, LANES), 1)
    unpack_ref[...] = jnp.where(token == slab_token(place), 1.0, 0.0).astype(BF16)
    row = lax.broadcasted_iota(jnp.int32, (ROWS, 128), 0)
    lane = lax.broadcasted_iota(jnp.int32, (ROWS, 128), 1)
    late = [(part >= WIN - SHIFT).astype(F32) for part in places(row)]
    value = jnp.zeros((ROWS, 128), F32)
    for axis in range(3):
        value = jnp.where(lane == 64 + 2 * axis, -BIG * (1.0 - late[axis]), value)
        value = jnp.where(lane == 65 + 2 * axis, -BIG * late[axis], value)
    value = jnp.where((lane == 70) & (row >= TOK), -BIG, value)
    kmask_ref[...] = value
    row = lax.broadcasted_iota(jnp.int32, (16, LANES), 0)
    lane = lax.broadcasted_iota(jnp.int32, (16, LANES), 1)
    late = [(part >= WIN - SHIFT).astype(F32) for part in places(lane)]
    value = jnp.where(row == 6, 1.0, 0.0)
    for axis in range(3):
        value = jnp.where(row == 2 * axis, late[axis], value)
        value = jnp.where(row == 2 * axis + 1, 1.0 - late[axis], value)
    qmask_ref[...] = value.astype(BF16)
    ones_ref[...] = spread_ones()
    heads = bias_ref.shape[0]
    for head in range(heads):
        row = jnp.broadcast_to(table_ref[head : head + 1, :], (8, TABLE))
        base_ref[...] = shear(row, -1)
        for first in range(WIN):
            for second in range(WIN):
                at = offset_of(first, second)
                rows = 8 * (first * WIN + second)
                wide_ref[rows : rows + 8, :] = base_ref[:, at : at + WIDE]
        high, mid, low = thirds(wide_ref[...])
        full = [
            (dot(high[:, a:b], ones_ref[a:b, c:d]) + dot(mid[:, a:b], ones_ref[a:b, c:d]))
            + dot(low[:, a:b], ones_ref[a:b, c:d])
            for a, b, c, d in ((0, LOW, 0, CUT), (HIGH, WIDE, CUT, LANES))
        ]
        full = jnp.concatenate(full, 1)
        for group in range(WIN * WIN):
            bias_ref[head, WIN * group : WIN * group + WIN, :] = full[8 * group : 8 * group + WIN]
        bias_ref[head, TOK:ROWS, :] = jnp.zeros((ROWS - TOK, LANES), F32)


def expand_table(table, w_qkv, b_qkv, gain, shift, heads, interpret=False):
    feats = w_qkv.shape[0]
    return pl.pallas_call(
        expand_body,
        out_shape=[
            jax.ShapeDtypeStruct((heads, ROWS, LANES), F32),
            jax.ShapeDtypeStruct((LANES, SLAB), BF16),
            jax.ShapeDtypeStruct((SLAB, LANES), BF16),
            jax.ShapeDtypeStruct((ROWS, 128), F32),
            jax.ShapeDtypeStruct((16, LANES), BF16),
            jax.ShapeDtypeStruct((128, 2 * heads * 128), BF16),
            jax.ShapeDtypeStruct((48 * heads + 2 * feats, HID), BF16),
            jax.ShapeDtypeStruct((feats, LANES), F32),
            jax.ShapeDtypeStruct((feats, LANES), F32),
        ],
        scratch_shapes=[
            pltpu.VMEM((8, TABLE), F32),
            pltpu.VMEM((WIDE, LANES), BF16),
            pltpu.VMEM((SLAB, WIDE), F32),
        ],
        cost_estimate=pl.CostEstimate(flops=4_000_000_000, bytes_accessed=2_000_000, transcendentals=0),
        compiler_params=pltpu.CompilerParams(vmem_limit_bytes=24 * 1024 * 1024),
        interpret=interpret,
        name="expand",
    )(table, w_qkv, b_qkv[None], gain[None], shift[None])


def column_sums(value):
    part = value[:, :128] + value[:, 128:256] + value[:, 256:]
    part = jnp.concatenate([part, jnp.zeros((128 - part.shape[0], 128), F32)], 0)
    return jnp.sum(part.T, 0, keepdims=True)


def fold_body(bit_ref, pairs_ref, gq_ref, gkv_ref, gproj_ref, vec_ref, keep_ref, send_ref, out_ref,
              all_ref, rows_ref, ones_ref, total_ref):
    feats = gproj_ref.shape[0]
    proj = jnp.concatenate([gproj_ref[...], jnp.zeros((HID - feats, feats), F32)], 0)
    all_ref[...] = jnp.concatenate([gq_ref[...], gkv_ref[...], proj], 1)
    for at in range(2):
        all_ref[feats + 1 + at : feats + 2 + at, :128] = column_sums(vec_ref[at])
    upper = bit_ref[0] == 1
    half = HID // 2
    keep_ref[...] = jnp.where(upper, all_ref[half:], all_ref[:half])
    send_ref[...] = jnp.where(upper, all_ref[:half], all_ref[half:])
    ones_ref[...] = spread_ones()
    heads = pairs_ref.shape[0]
    out_ref[...] = jnp.zeros(out_ref.shape, F32)
    rows_ref[...] = jnp.zeros(rows_ref.shape, F32)
    for head in range(heads):
        for group in range(WIN * WIN):
            rows_ref[head, 8 * group : 8 * group + WIN, :] = pairs_ref[head, WIN * group : WIN * group + WIN, :]
    for head in range(heads):
        high, low = halves(rows_ref[head])
        wide, rest = [
            dot(high[:, c:d], ones_ref[a:b, c:d], NT) + dot(low[:, c:d], ones_ref[a:b, c:d], NT)
            for a, b, c, d in ((0, LOW, 0, CUT), (HIGH, WIDE, CUT, LANES))
        ]
        wide = jnp.concatenate([wide[:, :HIGH], wide[:, HIGH:] + rest[:, : LOW - HIGH], rest[:, LOW - HIGH :]], 1)
        total_ref[head] = jnp.zeros(total_ref.shape[1:], F32)
        for first in range(WIN):
            for second in range(WIN):
                at = offset_of(first, second)
                rows = 8 * (first * WIN + second)
                total_ref[head, :, at : at + WIDE] = total_ref[head, :, at : at + WIDE] + wide[rows : rows + 8]
        entries = jnp.sum(shear(total_ref[head], 1), 0, keepdims=True)
        for part in range(TABLE // LANES):
            row = head * (TABLE // LANES) + part
            out_ref[row : row + 1, :] = entries[:, LANES * part : LANES * part + LANES]


def fold_sums(bit, sums):
    heads = sums[0].shape[0]
    rows = -(-heads * (TABLE // LANES) // 8) * 8
    half = jax.ShapeDtypeStruct((HID // 2, LANES), F32)
    return pl.pallas_call(
        fold_body,
        in_specs=[pl.BlockSpec(memory_space=pltpu.SMEM)] + [pl.BlockSpec(memory_space=pltpu.VMEM)] * 5,
        out_shape=[half, half, jax.ShapeDtypeStruct((rows, LANES), F32)],
        scratch_shapes=[
            pltpu.VMEM((HID, LANES), F32),
            pltpu.VMEM((heads, SLAB, LANES), F32),
            pltpu.VMEM((WIDE, LANES), BF16),
            pltpu.VMEM((heads, 8, TABLE), F32),
        ],
        cost_estimate=pl.CostEstimate(flops=3_000_000_000, bytes_accessed=2_000_000, transcendentals=0),
        compiler_params=pltpu.CompilerParams(vmem_limit_bytes=24 * 1024 * 1024),
        name="fold",
    )(bit, *sums)


def join_body(x_ref, d_ref, field_ref):
    feats = x_ref.shape[3]
    zero = jnp.zeros(field_ref.shape[:3] + (128 - feats,), BF16)
    field_ref[:, :, :, :128] = jnp.concatenate([x_ref[...], zero], -1)
    field_ref[:, :, :, 128:] = jnp.concatenate([d_ref[...], zero], -1)


def join_fields(inputs, d_out):
    rows = WIN if inputs.shape[0] % WIN == 0 else inputs.shape[0]
    block = (rows,) + inputs.shape[1:]
    spec = pl.BlockSpec(block, lambda i: (i, 0, 0, 0))
    return pl.pallas_call(
        join_body,
        grid=(inputs.shape[0] // rows,),
        in_specs=[spec, spec],
        out_specs=pl.BlockSpec(block[:3] + (256,), lambda i: (i, 0, 0, 0)),
        out_shape=jax.ShapeDtypeStruct(inputs.shape[:3] + (256,), BF16),
        compiler_params=pltpu.CompilerParams(vmem_limit_bytes=20 * 1024 * 1024),
        cost_estimate=pl.CostEstimate(flops=1_000_000_000, bytes_accessed=6_000_000, transcendentals=0),
        name="join",
    )(inputs, d_out)


def split_body(factor, bit_ref, part_ref, other_ref, entries_ref, gq_ref, gb_ref, gproj_ref, grel_ref, gain_ref, shift_ref):
    feats = gproj_ref.shape[0]
    wide = gq_ref.shape[1]
    upper = bit_ref[0] == 1
    low = jnp.where(upper, other_ref[...], part_ref[...])
    high = jnp.where(upper, part_ref[...], other_ref[...])
    full = jnp.concatenate([low, high], 0) * factor
    gq_ref[...] = full[:feats, :wide]
    gb_ref[...] = full[feats : feats + 1, :wide]
    gproj_ref[...] = full[:feats, wide:]
    gain_ref[...] = full[feats + 1 : feats + 2, :feats]
    shift_ref[...] = full[feats + 2 : feats + 3, :feats]
    per_head = TABLE // LANES
    for head in range(grel_ref.shape[0]):
        for part in range(per_head):
            lo = LANES * part
            hi = min(lo + LANES, grel_ref.shape[1])
            row = head * per_head + part
            grel_ref[head : head + 1, lo:hi] = entries_ref[row : row + 1, : hi - lo] * factor


def split_sums(factor, bit, part, other, entries, feats, heads, count):
    shapes = [(feats, 3 * feats), (1, 3 * feats), (feats, feats), (heads, count), (1, feats), (1, feats)]
    return pl.pallas_call(
        functools.partial(split_body, factor),
        in_specs=[pl.BlockSpec(memory_space=pltpu.SMEM)] + [pl.BlockSpec(memory_space=pltpu.VMEM)] * 3,
        out_shape=[jax.ShapeDtypeStruct(shape, F32) for shape in shapes],
        cost_estimate=pl.CostEstimate(flops=500_000_000, bytes_accessed=500_000, transcendentals=0),
        name="split",
    )(bit, part, other, entries)


def gather(field_ref, yhalo_ref, xhalo_ref, zhalo_ref, block_ref, base, last):
    row, col = pl.program_id(0), pl.program_id(1)
    at_x = WIN * (row + base) + SHIFT
    at_y = WIN * col + SHIFT
    edge = WIN - SHIFT
    last_col = col == pl.num_programs(1) - 1

    def own(first, count_x, second, count_y):
        spot = (pl.ds(at_x + first, count_x), pl.ds(at_y + second, count_y))
        block_ref[first : first + count_x, second : second + count_y, :WIN, :] = field_ref[spot].astype(F32)

    def arrived(first, count_x):
        block_ref[first : first + count_x, edge:, :WIN, :] = yhalo_ref[pl.ds(at_x + first, count_x)].astype(F32)

    def rows(first, count_x):
        own(first, count_x, 0, edge)

        @pl.when(last_col)
        def _():
            arrived(first, count_x)

        @pl.when(jnp.logical_not(last_col))
        def _():
            own(first, count_x, edge, SHIFT)

    if xhalo_ref is None:
        rows(0, WIN)
    else:
        last_row = row == pl.num_programs(0) - 1
        rows(0, edge)

        @pl.when(last_row)
        def _():
            block_ref[edge:, :, :WIN, :] = xhalo_ref[:, pl.ds(WIN * col, WIN)].astype(F32)

        @pl.when(jnp.logical_not(last_row))
        def _():
            rows(edge, SHIFT)

    block_ref[:, :, :SHIFT, :] = zhalo_ref[pl.ds(WIN * row, WIN), pl.ds(WIN * col, WIN)].astype(F32)


def window_body(base, has_xhalo, has_sums, *refs):
    refs = list(refs)
    flag_ref, field_ref, yhalo_ref, zhalo_ref = refs[:4]
    refs = refs[4:]
    xhalo_ref = refs.pop(0) if has_xhalo else None
    bias_ref, pack_ref, unpack_ref, kmask_ref, qmask_ref, wside_ref, wtrans_ref, gain_ref, shift_ref = refs[:9]
    wproj_ref, wqkv_ref = refs[9:11]
    refs = refs[11:]
    before = [refs.pop(0) for _ in range(5)] if has_sums else None
    dx_ref, pair_ref, gq_ref, gkv_ref, gproj_ref, vec_ref = refs[:6]
    (block_ref, score_ref, expo_ref, grad_ref, qdiag_ref, odiag_ref, kaug_ref, vaug_ref, attn_ref, dq_ref) = refs[6:]
    sums = (pair_ref, gq_ref, gkv_ref, gproj_ref, vec_ref)
    heads = pair_ref.shape[0]
    feats = wproj_ref.shape[0]
    hdim = feats // heads
    scale = hdim ** (-0.5)
    row, col = pl.program_id(0), pl.program_id(1)
    last = [
        ((row == pl.num_programs(0) - 1) if has_xhalo else False),
        col == pl.num_programs(1) - 1,
        True,
    ]

    @pl.when((row == 0) & (col == 0))
    def _():
        for at, ref in enumerate(sums):
            ref[...] = jnp.zeros(ref.shape, ref.dtype) if before is None else before[at][...]
        for ref in (block_ref, qdiag_ref, odiag_ref):
            ref[...] = jnp.zeros(ref.shape, ref.dtype)

    gather(field_ref, yhalo_ref, xhalo_ref, zhalo_ref, block_ref, base, last)
    block = block_ref[...].reshape(SLAB, 256).astype(BF16)
    packed = dot(pack_ref[...], block)
    dy_tok = packed[:, 128:].astype(BF16)
    x_t = packed[:, :128].T[:feats]
    dy_t = packed[:, 128:].T[:feats]
    mu = jnp.sum(x_t, 0, keepdims=True) * (1.0 / feats)
    centered = x_t - mu
    rstd = lax.rsqrt(jnp.sum(centered * centered, 0, keepdims=True) * (1.0 / feats) + 1e-05)
    xhat = centered * rstd
    valid = (lax.broadcasted_iota(jnp.int32, (1, LANES), 1) < TOK).astype(F32)
    normed = (xhat * gain_ref[...] + shift_ref[...]) * valid
    row = lax.broadcasted_iota(jnp.int32, (128 - feats, LANES), 0)
    tail = jnp.where(row < 3, valid, 0.0)
    norm_full = jnp.concatenate([normed, tail], 0)
    norm_t = norm_full[:HID].astype(BF16)
    norm_tok = norm_full.T[:ROWS].astype(BF16)

    lane = lax.broadcasted_iota(jnp.int32, (1, 128), 1)
    flags = jnp.where(lane == 70, 1.0, 0.0)
    for axis in range(3):
        edge = jnp.where(last[axis], flag_ref[axis], 0.0)
        flags = jnp.where((lane == 64 + 2 * axis) | (lane == 65 + 2 * axis), edge, flags)
    kmask = kmask_ref[...] * flags
    ones = jnp.where((lane >= 64) & (lane < 67), 1.0, 0.0)
    side = dot(norm_tok, wside_ref[...])
    for head in range(heads):
        kaug_ref[head] = (side[:, 128 * head : 128 * head + 128] + kmask).astype(BF16)
        base = 128 * (heads + head)
        vaug_ref[head] = (side[:, base : base + 128] + ones).astype(BF16)
    turned = dot(wtrans_ref[...], norm_t)
    q_at = 48 * heads
    k_at = q_at + feats
    q_t = turned[q_at : q_at + feats].astype(BF16)
    k_t = turned[k_at : k_at + feats].astype(BF16)
    do_t = dot(wproj_ref[...], dy_tok[:, :feats], NT).astype(BF16).astype(F32)
    scaled = q_t.astype(F32) * (scale * 1.4426950408889634)

    spans = [slice(LANES * head, LANES * (head + 1)) for head in range(heads)]
    parts = [slice(hdim * head, hdim * (head + 1)) for head in range(heads)]
    tops, o_augs = [], []
    for head in range(heads):
        q_high, q_low = halves(scaled[parts[head]])
        q_aug = jnp.concatenate([q_high, q_low, qmask_ref[...]], 0)
        score = dot(kaug_ref[head, :, :AUG], q_aug) + bias_ref[head]
        score_ref[head] = score
        tops.append(jnp.max(score, 0, keepdims=True))
    for head in range(heads):
        expo = jnp.exp2(score_ref[head] - tops[head]).astype(BF16)
        expo_ref[:, spans[head]] = expo
        v_t = turned[48 * head : 48 * head + 48].astype(BF16)
        out = dot(v_t[:, :ROWS], expo_ref[:, spans[head]])
        inverse = 1.0 / out[hdim : hdim + 1]
        out = out[:hdim] * inverse
        attn_ref[parts[head], :] = out.astype(BF16)
        grad_out = do_t[parts[head]]
        mean = jnp.sum(out * grad_out, 0, keepdims=True) * (-inverse)
        o_high, o_low = halves(grad_out * inverse)
        odiag_ref[parts[head], spans[head]] = o_high
        qdiag_ref[parts[head], spans[head]] = q_t[parts[head]]
        m_high, m_mid, m_low = thirds(mean)
        row16 = lax.broadcasted_iota(jnp.int32, (16, LANES), 0)
        m_rows = jnp.where(
            row16 == 0,
            m_high.astype(F32),
            jnp.where(row16 == 1, m_mid.astype(F32), jnp.where(row16 == 2, m_low.astype(F32), 0.0)),
        ).astype(BF16)
        o_augs.append(jnp.concatenate([o_high, o_low, m_rows], 0))
    dv = dot(expo_ref[...], odiag_ref[...], NT).astype(BF16)
    for head in range(heads):
        grads = dot(vaug_ref[head, :, :AUG], o_augs[head]) * expo_ref[:, spans[head]].astype(F32)
        pair_ref[head] = pair_ref[head] + grads
        grad_ref[:, spans[head]] = grads.astype(BF16)
    for head in range(heads):
        dq_ref[parts[head], :] = (dot(k_t[parts[head], :ROWS], grad_ref[:, spans[head]]) * scale).astype(BF16)

    dk = (dot(grad_ref[...], qdiag_ref[...], NT) * scale).astype(BF16)
    dkv = jnp.concatenate([dk, dv], 1)
    dq = dq_ref[...]
    gq_ref[...] = gq_ref[...] + dot(norm_t, dq, NT)
    gkv_ref[...] = gkv_ref[...] + dot(norm_t[:, :ROWS], dkv)
    gproj_ref[...] = gproj_ref[...] + dot(attn_ref[...], dy_tok[:, :feats])
    dkv_all = jnp.concatenate([dkv, jnp.zeros((LANES - ROWS, 2 * feats), BF16)], 0)
    grad_in = dot(wqkv_ref[:, :feats], dq) + dot(wqkv_ref[:, feats:], dkv_all, NT)
    vec_ref[0] = vec_ref[0] + grad_in * xhat
    vec_ref[1] = vec_ref[1] + grad_in
    dhat = grad_in * gain_ref[...]
    mean_one = jnp.sum(dhat, 0, keepdims=True) * (1.0 / feats)
    mean_two = jnp.sum(dhat * xhat, 0, keepdims=True) * (1.0 / feats)
    d_x = (dy_t + rstd * (dhat - mean_one - xhat * mean_two)).astype(BF16)
    spread = dot(unpack_ref[...], d_x, NT)
    dx_ref[...] = spread.reshape(WIN, WIN, 8, feats).astype(BF16)


def window_call(base, count, flags, field, yhalo, zhalo, xhalo, tables, weights, sums, heads, interpret=False):
    cells_y, feats = field.shape[1], weights[0].shape[0]
    grid = (count, cells_y // WIN)

    def whole(_):
        return pl.BlockSpec(memory_space=pltpu.VMEM)

    arrays = [field, yhalo, zhalo] + ([] if xhalo is None else [xhalo])
    arrays += list(tables) + list(weights) + ([] if sums is None else list(sums))
    shapes = [(heads, ROWS, LANES), (HID, feats), (HID, 2 * feats), (feats, feats), (2, feats, LANES)]
    shapes = [jax.ShapeDtypeStruct(shape, F32) for shape in shapes]
    return pl.pallas_call(
        functools.partial(window_body, base, xhalo is not None, sums is not None),
        grid=grid,
        in_specs=[pl.BlockSpec(memory_space=pltpu.SMEM)] + [whole(a) for a in arrays],
        out_specs=[pl.BlockSpec((WIN, WIN, 8, feats), lambda i, j: (i, j, 0, 0))] + [whole(s) for s in shapes],
        out_shape=[jax.ShapeDtypeStruct((WIN * count, cells_y, 8, feats), BF16)] + shapes,
        scratch_shapes=[
            pltpu.VMEM((WIN, WIN, 8, 256), F32),
            pltpu.VMEM((heads, ROWS, LANES), F32),
            pltpu.VMEM((ROWS, heads * LANES), BF16),
            pltpu.VMEM((ROWS, heads * LANES), BF16),
            pltpu.VMEM((feats, heads * LANES), BF16),
            pltpu.VMEM((feats, heads * LANES), BF16),
            pltpu.VMEM((heads, ROWS, 128), BF16),
            pltpu.VMEM((heads, ROWS, 128), BF16),
            pltpu.VMEM((feats, LANES), BF16),
            pltpu.VMEM((feats, LANES), BF16),
        ],
        compiler_params=pltpu.CompilerParams(
            dimension_semantics=("arbitrary",) * 2, vmem_limit_bytes=32 * 1024 * 1024
        ),
        cost_estimate=pl.CostEstimate(
            flops=2_200_000_000 * count * grid[1], bytes_accessed=8_000_000, transcendentals=0
        ),
        interpret=interpret,
        name="windows",
    )(flags, *arrays)


def shifted(block, axis, distance):
    count = lax.axis_size(axis)
    return lax.ppermute(block, axis, [((i - distance) % count, i) for i in range(count)])


def crossed(block, axes, masks):
    sizes = [lax.axis_size(axis) for axis in axes]
    route = []
    for place in itertools.product(*map(range, sizes)):
        other = [at ^ masks.get(axis, 0) for at, axis in zip(place, axes)]
        source = target = 0
        for size, at, to in zip(sizes, place, other):
            source, target = source * size + at, target * size + to
        route.append((source, target))
    return lax.ppermute(block, axes, route)


def exchanged(part, axes):
    bits = []
    for axis in (axes[2], axes[1], axes[0]):
        size = lax.axis_size(axis)
        if size & (size - 1):
            part = lax.psum(part, axis)
            continue
        step = 2 if axis == axes[1] else 1
        while step < size:
            bits.append((axis, step))
            step *= 2
    while bits:
        one = bits.pop(0)
        if not bits:
            part = part + crossed(part, axes, dict([one]))
            break
        two = bits.pop(0)
        joined = {one[0]: one[1]}
        joined[two[0]] = joined.get(two[0], 0) + two[1]
        near, far, both = (crossed(part, axes, masks) for masks in (dict([one]), dict([two]), joined))
        part = (part + near) + (far + both)
    return part


def shards(inputs, d_out, layer_norm_gain, layer_norm_bias, w_qkv, b_qkv, w_proj, rel_bias):
    cells_x, cells_y, cells_z, feats = inputs.shape
    heads = rel_bias.shape[0]
    axes = ("gx", "gy", "gz")
    rows = cells_x // WIN
    counts = [1, rows - 2, 1] if rows > 2 else [rows]
    bases = [sum(counts[:i]) for i in range(len(counts))]

    field = join_fields(inputs, d_out)
    direct = shifted(field[SHIFT : WIN + SHIFT, SHIFT:, :SHIFT], "gz", -1)
    yhalo = shifted(field[:, :SHIFT], "gy", -1)

    def layers(lo, hi, depth):
        return jnp.concatenate([field[lo:hi, SHIFT:, :depth], yhalo[lo:hi, :, :depth]], 1)

    lo, hi = SHIFT, WIN * counts[0] + SHIFT
    zhalos = []
    xsend = layers(0, SHIFT, cells_z)
    if hi <= cells_x:
        corner = yhalo[lo:hi, :, :SHIFT]
        corner, xsend, rel_bias = lax.optimization_barrier((corner, xsend, rel_bias))
        zhalos.append(jnp.concatenate([direct, shifted(corner, "gz", -1)], 1))
    xhalo = shifted(xsend, "gx", -1)
    table = jnp.pad(rel_bias * 1.4426950408889634, ((0, 8 - heads), (0, TABLE - rel_bias.shape[1])))
    tables = list(expand_table(table, w_qkv, b_qkv, layer_norm_gain, layer_norm_bias, heads))
    for base, count in list(zip(bases, counts))[len(zhalos) :]:
        lo, hi = WIN * base + SHIFT, WIN * (base + count) + SHIFT
        edge = layers(lo, min(hi, cells_x), SHIFT)
        if hi > cells_x:
            edge = jnp.concatenate([edge, xhalo[:, :, :SHIFT]], 0)
        zhalos.append(shifted(edge, "gz", -1))
    weights = (w_proj, w_qkv)
    flags = jnp.stack([(lax.axis_index(a) == lax.axis_size(a) - 1).astype(F32) for a in axes])
    sums, fields = None, []
    for at, (base, count) in enumerate(zip(bases, counts)):
        last = at == len(counts) - 1
        part, *sums = window_call(
            base, count, flags, field, yhalo, zhalos[at], xhalo if last else None, tables, weights,
            sums, heads,
        )
        edge = part[:, :, :SHIFT]
        if last:
            edge, sums[0] = lax.optimization_barrier((edge, sums[0]))
        arrived = shifted(edge, "gz", 1)
        fields.append(jnp.concatenate([arrived, part[:, :, SHIFT:cells_z]], 2))
    paired = lax.axis_size("gy") % 2 == 0
    bit = lax.axis_index("gy") & 1 if paired else jnp.zeros((), jnp.int32)
    keep, send, entries = fold_sums(bit.reshape(1), sums)
    near = {"gy": 1}
    if not paired:
        part, other, entries = lax.psum((keep, send, entries), axes)
    else:
        part = jnp.concatenate([keep + crossed(send, axes, near), entries + crossed(entries, axes, near)], 0)
        part = exchanged(part, axes)
        part, entries = part[: HID // 2], part[HID // 2 :]
        other = crossed(part, axes, near)
    arrived = shifted(fields[-1][-SHIFT:], "gx", 1)
    d_x = jnp.concatenate([arrived] + fields[:-1] + [fields[-1][:-SHIFT]], 0)
    edge = cells_y - SHIFT
    d_x = jnp.concatenate([shifted(d_x[:, edge:], "gy", 1), d_x[:, :edge]], 1)
    count = inputs.shape[0] * inputs.shape[1] * inputs.shape[2]
    for a in axes:
        count *= lax.axis_size(a)
    g_qkv, g_bias, g_proj, g_rel, g_gain, g_shift = split_sums(
        float(count) ** (-0.5), bit.reshape(1), part, other, entries, feats, heads, rel_bias.shape[1]
    )
    return d_x, g_qkv, g_bias.reshape(-1), g_proj, g_rel, g_gain.reshape(-1), g_shift.reshape(-1)


def solution(mesh):
    placed = (P("gx", "gy", "gz", None), P("gx", "gy", "gz", None), P(), P(), P(), P(), P(), P())
    return jax.shard_map(
        shards,
        mesh=mesh,
        in_specs=placed,
        out_specs=(P("gx", "gy", "gz", None), P(), P(), P(), P(), P(), P()),
        check_vma=False,
    )
```
